32 devices in a mesh: dp: 8 (over z, x), mp: 4 (over y, core).
Axes of the slice: x: 2, y: 2, z: 4, core: 2. Of those that a mesh axis runs over, the one named last changes fastest.
Arguments:
- hidden: bfloat16 [2304, 5376], P('dp', 'mp'), may hold values from -6 to 6
- master: float32 [5376, 4096], P(('mp', 'dp')), may hold values from -0.078125 to 0.078125
- grad: float32 [5376, 4096], P(('mp', 'dp')), may hold values from -1500 to 1500, as said below
- row_factor: float32 [5376], P(('mp', 'dp')), may hold values from 0.01 to 1, as said below
- col_factor: float32 [4096], replicated, may hold values from 0.05 to 0.5
Outputs:
- ffn_out: bfloat16 [2304, 4096], P('dp', 'mp')
- update: float32 [5376, 4096], P(('mp', 'dp'))
- row_new: float32 [5376], P(('mp', 'dp'))
- col_new: float32 [4096], replicated
The draws below stay inside these ranges and needn't reach their ends.
Inputs may be any that keep to these rules, and one draw needn't show every extreme that they name: `grad`: every entry is finite. `row_factor`: every entry is positive.
All inputs are finite; a program needn't handle non-finite values.
Results may differ from the reference program's by a relative error of at most 0.0049.
Values may be sent and summed in bfloat16 or wider, within the bound.
A program may use at most 64 MiB of HBM per device.

```python
import math
import jax
import jax.numpy as jnp
from jax import lax

D = 4096
FFW = 5376
STEP = 10
TOKENS = 2304
N_DP = 8
N_MP = 4


def draw_grad(key, part):
    key_base = jax.random.fold_in(key, 101)
    key_rows = jax.random.fold_in(key, 102)
    key_cols = jax.random.fold_in(key, 103)
    key_perm = jax.random.fold_in(key, 104)
    base = jnp.clip(jax.random.normal(key_base, (FFW, D), jnp.float32), -6.0, 6.0)
    low = jnp.log(0.3)
    high = jnp.log(3.0)
    row_scale = jnp.exp(jax.random.uniform(key_rows, (FFW, 1), jnp.float32, low, high))
    ramp = jnp.sqrt(1.0 + 2.0 * jnp.arange(FFW, dtype=jnp.float32)[:, None] / (FFW - 1))
    col_scale = jnp.exp(jax.random.uniform(key_cols, (1, D), jnp.float32, low, high))
    blocks = N_DP * N_MP
    group = FFW // blocks
    order = jax.random.permutation(key_perm, blocks)
    owner = order[jnp.arange(FFW) // group]
    marked = jnp.arange(D)[None, :] % blocks == owner[:, None]
    spike = jnp.where(marked, 30.0, 1.0)
    return (0.5 * base * row_scale * ramp * col_scale * spike).astype(jnp.float32)


def draw_row_factor(key, part):
    key_rough = jax.random.fold_in(key, 201)
    rough = jnp.exp(jax.random.uniform(key_rough, (FFW,), jnp.float32, jnp.log(0.1), 0.0))
    ramp = jnp.exp(-jnp.log(9.0) * jnp.arange(FFW, dtype=jnp.float32) / (FFW - 1))
    return (rough * ramp).astype(jnp.float32)


def block_scale(own_key, dims, cuts, smallest, top_value):
    def one(dim, shards_of):
        draws = jax.random.uniform(jax.random.fold_in(jax.random.fold_in(own_key, 6), dim), (shards_of,), jnp.float32, smallest / len(cuts), top_value / len(cuts))
        return jnp.repeat(jnp.exp(draws), dims[dim] // shards_of).reshape((-1,) + (1,) * (len(dims) - dim - 1))

    loudness = one(*cuts[0])
    for cut in cuts[1:]:
        loudness = loudness * one(*cut)
    return loudness


def gaussian(key, shape, spread, limit, split=(), held_as=jnp.bfloat16):
    result = spread * jax.random.normal(key, shape, jnp.float32)
    if split:
        result = result * block_scale(key, shape, split, -0.22, 0.18)
    return jnp.clip(result, -limit, limit).astype(held_as)


def setup_inputs(seed: int = 0) -> dict:
    streams_of = jax.random.split(jax.random.key(seed), 6)
    return {
        "hidden": gaussian(streams_of[0], (TOKENS, FFW), 1.0, 6.0, ((0, 8), (1, 4))),
        "master": gaussian(streams_of[1], (FFW, D), FFW ** -0.5, 0.078125, ((0, 32),), jnp.float32),
        "grad": draw_grad(jax.random.fold_in(streams_of[5], 71), 0),
        "row_factor": draw_row_factor(jax.random.fold_in(streams_of[5], 71), 0),
        "col_factor": jnp.clip(jnp.exp(jax.random.uniform(streams_of[4], (D,), jnp.float32, math.log(0.05), math.log(0.5))), 0.05, 0.5),
    }


def reference(hidden, master, grad, row_factor, col_factor):
    keep = 1.0 - STEP ** (-0.8)
    step_rate = min(0.01, STEP ** (-0.5))
    squared = grad * grad + 1e-30
    row_new = keep * row_factor + (1.0 - keep) * lax.optimization_barrier(jnp.mean(squared, axis=1))
    col_new = keep * col_factor + (1.0 - keep) * lax.optimization_barrier(jnp.mean(squared, axis=0))
    scaled = grad * lax.rsqrt(row_new[:, None] * col_new[None, :])
    root_mean = jnp.sqrt(jnp.mean(scaled * scaled))
    update = scaled / jnp.maximum(1.0, root_mean)
    weight = (master - step_rate * update).astype(jnp.bfloat16)
    ffn_out = jnp.dot(hidden, weight, preferred_element_type=jnp.float32).astype(jnp.bfloat16)
    return (ffn_out, update, row_new, col_new)
```

```python
import functools

import jax
import jax.numpy as jnp
from jax import lax
from jax.experimental import pallas as pl
from jax.experimental.pallas import tpu as pltpu
from jax.sharding import PartitionSpec as P

D = 4096
FFW = 5376
STEP = 10
KEEP = 1.0 - STEP ** (-0.8)
RATE = min(0.01, STEP ** (-0.5))
MESH = pl.DeviceIdType.MESH
NX = 2
NZ = 4
NC = 4


def up(n, m):
    return (n + m - 1) // m * m


def kernel(
    hid_ref, master_ref, grad_ref, rf_ref, cf_ref,
    out_ref, upd_ref, row_ref, col_ref,
    hfull, wsend, wfull, acc, wacc, statz, statp, mult, psend, precv,
    s_statz, r_statz, s_statp, r_statp, s_hz, r_hz, s_hy, r_hy, s_hc, r_hc, s_w, r_w, s_p, r_p,
):
    rows, d = grad_ref.shape
    tok = hid_ref.shape[1]
    kp = hid_ref.shape[2]
    rp = wsend.shape[2]
    cw = wsend.shape[3]
    nb = NC * cw
    ffw = rows * NX * NZ * 4
    dp = lax.axis_index("dp")
    mp = lax.axis_index("mp")
    z, x = dp // NX, dp % NX
    y, c = mp // 2, mp % 2

    def dev(z_=None, x_=None, mp_=None):
        z_ = z if z_ is None else z_
        x_ = x if x_ is None else x_
        mp_ = mp if mp_ is None else mp_
        return {"dp": z_ * NX + x_, "mp": mp_}

    def flip(dy, dc):
        return (y + dy) % 2 * 2 + (c + dc) % 2

    def copy(src, dst, ssem, rsem, to):
        return pltpu.make_async_remote_copy(
            src_ref=src, dst_ref=dst, send_sem=ssem, recv_sem=rsem, device_id=to, device_id_type=MESH
        )

    zpeers = [(z + k) % NZ for k in range(1, NZ)]
    layer = [(dx, dy, dc) for dx in range(2) for dy in range(2) for dc in range(2)][1:]
    barrier = pltpu.get_barrier_semaphore()
    for zz in zpeers:
        pl.semaphore_signal(barrier, inc=1, device_id=dev(z_=zz), device_id_type=MESH)
    for dx, dy, dc in layer:
        pl.semaphore_signal(
            barrier, inc=1, device_id=dev(x_=(x + dx) % 2, mp_=flip(dy, dc)), device_id_type=MESH
        )

    acc[...] = jnp.zeros_like(acc)
    wacc[...] = jnp.zeros_like(wacc)

    def stat_step(i, carry):
        r = pl.ds(pl.multiple_of(i * 8, 8), 8)
        g = grad_ref[r, :]
        g2 = g * g
        sq = g2 + 1e-30
        rn = KEEP * rf_ref[r, :] + (1.0 - KEEP) * (jnp.sum(sq, axis=1, keepdims=True) / float(d))
        row_ref[r, :] = rn
        acc[...] += sq
        wacc[...] += g2 * (1.0 / rn)
        return carry

    lax.fori_loop(0, rows // 8, stat_step, 0)
    pa = jnp.sum(acc[...], axis=0, keepdims=True)
    pw = jnp.sum(wacc[...], axis=0, keepdims=True)
    q = d // 4
    for j in range(4):
        statz[z, j : j + 1, :] = pa[:, j * q : (j + 1) * q]
        statz[z, 4 + j : 5 + j, :] = pw[:, j * q : (j + 1) * q]
    wsend[...] = jnp.zeros_like(wsend)
    for k in range(NC):
        for m in range(4):
            wfull[k, m * kp + 2 * rp : (m + 1) * kp, :] = jnp.zeros((kp - 2 * rp, cw), wfull.dtype)

    pl.semaphore_wait(barrier, NZ - 1 + 7)

    stz = [
        copy(statz.at[z], statz.at[z], s_statz.at[k], r_statz.at[k], dev(z_=zz))
        for k, zz in enumerate(zpeers)
    ]
    for s in stz:
        s.start()
    my_lane = pl.ds(pl.multiple_of(mp * kp, 128), kp)
    hz = [
        copy(hid_ref.at[zz], hfull.at[z, :, my_lane], s_hz.at[k], r_hz.at[k], dev(z_=zz))
        for k, zz in enumerate(zpeers)
    ]
    for h in hz:
        h.start()
    hfull[z, :, my_lane] = hid_ref[z]
    for s in stz:
        s.wait()
    total = ((statz[0] + statz[1]) + statz[2]) + statz[3]
    for k, to in enumerate((dev(mp_=flip(1, 0)), dev(x_=1 - x), dev(mp_=flip(0, 1)))):
        statp[k, 0] = total
        s = copy(statp.at[k, 0], statp.at[k, 1], s_statp.at[k], r_statp.at[k], to)
        s.start()
        s.wait()
        total = total + statp[k, 1]
    for j in range(4):
        cols = slice(j * q, (j + 1) * q)
        col_ref[:, cols] = KEEP * cf_ref[:, cols] + (1.0 - KEEP) * total[j : j + 1, :] / float(ffw)
        acc[0:1, cols] = total[4 + j : 5 + j, :]
    square_total = jnp.sum(acc[0:1, :] / col_ref[...], axis=1, keepdims=True)
    root_mean = jnp.sqrt(square_total / float(ffw * d))
    mult[...] = 1.0 / jnp.maximum(1.0, root_mean)

    my_rows = pl.ds(pl.multiple_of(mp * kp + x * rp, 16), rp)

    def w_copy(k, n):
        dx, dy, dc = layer[n]
        j = flip(dy, dc)
        return copy(
            wsend.at[k, j], wfull.at[k, my_rows, :], s_w.at[k, n], r_w.at[k, n],
            dev(x_=(x + dx) % 2, mp_=j),
        )

    def weights(k, carry):
        def block(j, carry):
            cols = pl.ds(pl.multiple_of(j * nb + k * cw, 128), cw)
            scaled = grad_ref[:, cols] * lax.rsqrt(row_ref[...] * col_ref[:, cols])
            u = scaled * mult[...]
            upd_ref[:, cols] = u
            wsend[k, j, 0:rows, :] = (master_ref[:, cols] - RATE * u).astype(jnp.bfloat16)
            return carry

        lax.fori_loop(0, 4, block, 0)
        for n in range(len(layer)):
            w_copy(k, n).start()
        wfull[k, my_rows, :] = wsend[k, mp]
        return carry

    lax.fori_loop(0, NC, weights, 0)

    other_lane = pl.ds(pl.multiple_of(flip(1, 0) * kp, 128), kp)
    order = [z] + [(z - k) % NZ for k in range(1, NZ)]
    hy, hc = [], []
    for k, t in enumerate(order):
        if k:
            hz[k - 1].wait_recv()
        part = hfull.at[t, :, my_lane]
        hy.append(copy(part, part, s_hy.at[k], r_hy.at[k], dev(mp_=flip(1, 0))))
        hc.append(copy(part, part, s_hc.at[0, k], r_hc.at[0, k], dev(mp_=flip(0, 1))))
        hy[-1].start()
        hc[-1].start()
    for k, t in enumerate(order):
        hy[k].wait_recv()
        part = hfull.at[t, :, other_lane]
        hc.append(copy(part, part, s_hc.at[1, k], r_hc.at[1, k], dev(mp_=flip(0, 1))))
        hc[-1].start()
    for h in hc:
        h.wait_recv()

    def product(k, t):
        return jnp.dot(hfull[t], wfull[k], preferred_element_type=jnp.float32)

    def p_copy(k, way, dist):
        step = 1 if way == 0 else -1
        slot = way * 3 + (dist - 1)
        land = slot
        return copy(
            psend.at[k, slot], precv.at[k, land], s_p.at[k, slot], r_p.at[k, land],
            dev(z_=jnp.clip(z + step, 0, NZ - 1)),
        )

    def p_wait(k, way, dist):
        slot = way * 3 + dist - 1
        copy(psend.at[k, slot], precv.at[k, slot], s_p.at[k, slot], r_p.at[k, slot], dev(z_=(z + 1) % NZ)).wait_recv()

    def inside(way, dist):
        return z + dist <= NZ - 1 if way == 0 else z - dist >= 0

    def has_before(way):
        return z > 0 if way == 0 else z < NZ - 1

    def send_step(k, carry):
        for n in range(len(layer)):
            w_copy(k, n).wait_recv()
        for dist in range(NZ - 1, 0, -1):
            for way in range(2):
                @pl.when(inside(way, dist))
                def _():
                    t = z + dist if way == 0 else z - dist
                    part = product(k, t)
                    slot = way * 3 + dist - 1
                    if dist < NZ - 1:
                        @pl.when(has_before(way))
                        def _():
                            p_wait(k, way, dist + 1)
                            psend[k, slot] = (part + precv[k, slot + 1].astype(jnp.float32)).astype(jnp.bfloat16)

                        @pl.when(jnp.logical_not(has_before(way)))
                        def _():
                            psend[k, slot] = part.astype(jnp.bfloat16)
                    else:
                        psend[k, slot] = part.astype(jnp.bfloat16)
                    p_copy(k, way, dist).start()
        return carry

    lax.fori_loop(0, NC, send_step, 0)

    for k in range(NC):
        cols = slice(k * cw, (k + 1) * cw)
        acc2 = product(k, z)
        for way in range(2):
            @pl.when(has_before(way))
            def _():
                p_wait(k, way, 1)

            acc2 = acc2 + jnp.where(has_before(way), precv[k, way * 3].astype(jnp.float32), 0.0)
        out_ref[:, cols] = acc2.astype(out_ref.dtype)

    def drain(k, carry):
        for n in range(len(layer)):
            w_copy(k, n).wait_send()
        for dist in range(NZ - 1, 0, -1):
            for way in range(2):
                @pl.when(inside(way, dist))
                def _():
                    p_copy(k, way, dist).wait_send()
        return carry

    lax.fori_loop(0, NC, drain, 0)
    for h in hz + hy + hc:
        h.wait_send()


def fast_body(hidden, master, grad, row_factor, col_factor):
    tok, kin = hidden.shape
    rows, d = grad.shape
    rp = up(rows, 16)
    kp = up(NX * rp, 128)
    nb = d // 4
    cw = nb // NC
    h = hidden.reshape(tok, NZ, NX, rows)
    h = jnp.pad(h, ((0, 0), (0, 0), (0, 0), (0, rp - rows))).reshape(tok, NZ, NX * rp)
    h = jnp.pad(h, ((0, 0), (0, 0), (0, kp - NX * rp))).transpose(1, 0, 2)
    dma = pltpu.SemaphoreType.DMA
    bf, f32 = jnp.bfloat16, jnp.float32
    vmem = pl.BlockSpec(memory_space=pltpu.VMEM)
    out, upd, row, col = pl.pallas_call(
        kernel,
        out_shape=(
            jax.ShapeDtypeStruct((tok, nb), bf),
            jax.ShapeDtypeStruct((rows, d), f32),
            jax.ShapeDtypeStruct((rows, 1), f32),
            jax.ShapeDtypeStruct((1, d), f32),
        ),
        in_specs=[vmem] * 5,
        out_specs=(vmem,) * 4,
        scratch_shapes=[
            pltpu.VMEM((NZ, tok, 4 * kp), bf),
            pltpu.VMEM((NC, 4, rp, cw), bf),
            pltpu.VMEM((NC, 4 * kp, cw), bf),
            pltpu.VMEM((8, d), f32),
            pltpu.VMEM((8, d), f32),
            pltpu.VMEM((NZ, 8, d // 4), f32),
            pltpu.VMEM((3, 2, 8, d // 4), f32),
            pltpu.VMEM((1, 1), f32),
            pltpu.VMEM((NC, 6, tok, cw), bf),
            pltpu.VMEM((NC, 6, tok, cw), bf),
            dma((3,)), dma((3,)), dma((3,)), dma((3,)),
            dma((3,)), dma((3,)), dma((4,)), dma((4,)), dma((2, 4)), dma((2, 4)),
            dma((NC, 7)), dma((NC, 7)), dma((NC, 6)), dma((NC, 6)),
        ],
        compiler_params=pltpu.CompilerParams(
            collective_id=0, has_side_effects=True, vmem_limit_bytes=60 * 1024 * 1024
        ),
    )(h, master, grad, row_factor[:, None], col_factor[None, :])
    return out, upd, row[:, 0], col[0]


def plain_body(hidden, master, grad, row_factor, col_factor):
    squared = grad * grad + 1e-30
    row_new = KEEP * row_factor + (1.0 - KEEP) * jnp.mean(squared, axis=1)
    column_part = jnp.sum(squared, axis=0)
    weighted_part = jnp.sum(grad * grad / row_new[:, None], axis=0)
    column_total, weighted_total = lax.psum((column_part, weighted_part), ("dp", "mp"))
    col_new = KEEP * col_factor + (1.0 - KEEP) * column_total / float(FFW)
    scaled = grad * lax.rsqrt(row_new[:, None] * col_new[None, :])
    root_mean = jnp.sqrt(jnp.sum(weighted_total / col_new) / float(FFW * D))
    update = scaled / jnp.maximum(1.0, root_mean)
    weight = (master - RATE * update).astype(jnp.bfloat16)
    partial_out = jnp.dot(
        hidden, lax.all_gather(weight, "dp", axis=0, tiled=True), preferred_element_type=jnp.float32
    )
    ffn_out = lax.psum_scatter(partial_out, "mp", scatter_dimension=1, tiled=True)
    return ffn_out.astype(jnp.bfloat16), update, row_new, col_new


def solution(mesh):
    fits = mesh.shape["dp"] == NX * NZ and mesh.shape["mp"] == 4
    return jax.shard_map(
        fast_body if fits else plain_body,
        mesh=mesh,
        in_specs=(
            P("dp", "mp"),
            P(("mp", "dp"), None),
            P(("mp", "dp"), None),
            P(("mp", "dp")),
            P(),
        ),
        out_specs=(P("dp", "mp"), P(("mp", "dp"), None), P(("mp", "dp")), P()),
        check_vma=False,
    )
```

```python
import functools

import jax
import jax.numpy as jnp
from jax import lax
from jax.experimental import pallas as pl
from jax.experimental.pallas import tpu as pltpu
from jax.sharding import PartitionSpec as P

D = 4096
FFW = 5376
STEP = 10
KEEP = 1.0 - STEP ** (-0.8)
RATE = min(0.01, STEP ** (-0.5))
MESH = pl.DeviceIdType.MESH
NX = 2
NZ = 4
NC = 4


def up(n, m):
    return (n + m - 1) // m * m


def kernel(
    hid_ref, master_ref, grad_ref, rf_ref, cf_ref,
    out_ref, upd_ref, row_ref, col_ref,
    hfull, wsend, wfull, acc, wacc, statz, statp, mult, psend, precv,
    s_statz, r_statz, s_statp, r_statp, s_hz, r_hz, s_hy, r_hy, s_hc, r_hc, s_w, r_w, s_p, r_p,
):
    rows, d = grad_ref.shape
    tok = hid_ref.shape[1]
    kp = hid_ref.shape[2]
    rp = wsend.shape[2]
    cw = wsend.shape[3]
    nb = NC * cw
    ffw = rows * NX * NZ * 4
    dp = lax.axis_index("dp")
    mp = lax.axis_index("mp")
    z, x = dp // NX, dp % NX
    y, c = mp // 2, mp % 2

    def dev(z_=None, x_=None, mp_=None):
        z_ = z if z_ is None else z_
        x_ = x if x_ is None else x_
        mp_ = mp if mp_ is None else mp_
        return {"dp": z_ * NX + x_, "mp": mp_}

    def flip(dy, dc):
        return (y + dy) % 2 * 2 + (c + dc) % 2

    def copy(src, dst, ssem, rsem, to):
        return pltpu.make_async_remote_copy(
            src_ref=src, dst_ref=dst, send_sem=ssem, recv_sem=rsem, device_id=to, device_id_type=MESH
        )

    zpeers = [(z + k) % NZ for k in range(1, NZ)]
    turns = [(0, 1), (1, 0), (1, 1)]
    barrier = pltpu.get_barrier_semaphore()
    for zz in zpeers:
        pl.semaphore_signal(barrier, inc=1, device_id=dev(z_=zz), device_id_type=MESH)
    for turn in turns:
        pl.semaphore_signal(barrier, inc=1, device_id=dev(mp_=flip(*turn)), device_id_type=MESH)
    pl.semaphore_signal(barrier, inc=1, device_id=dev(x_=1 - x), device_id_type=MESH)

    my_lane = pl.ds(pl.multiple_of(mp * kp, 128), kp)
    hfull[z, :, my_lane] = hid_ref[z]
    order = [z] + [(z - k) % NZ for k in range(1, NZ)]
    hz = [
        copy(hid_ref.at[zz], hfull.at[z, :, my_lane], s_hz.at[k], r_hz.at[k], dev(z_=zz))
        for k, zz in enumerate(zpeers)
    ]
    hy, hc = [], []

    def relay(k):
        if k:
            hz[k - 1].wait_recv()
        part = hfull.at[order[k], :, my_lane]
        hy.append(copy(part, part, s_hy.at[k], r_hy.at[k], dev(mp_=flip(1, 0))))
        hc.append(copy(part, part, s_hc.at[0, k], r_hc.at[0, k], dev(mp_=flip(0, 1))))
        hy[-1].start()
        hc[-1].start()

    pl.semaphore_wait(barrier, NZ - 1 + 4)
    hz[0].start()
    relay(0)

    acc[...] = jnp.zeros_like(acc)
    wacc[...] = jnp.zeros_like(wacc)

    def stat_step(i, carry):
        r = pl.ds(pl.multiple_of(i * 8, 8), 8)
        g = grad_ref[r, :]
        g2 = g * g
        sq = g2 + 1e-30
        rn = KEEP * rf_ref[r, :] + (1.0 - KEEP) * (jnp.sum(sq, axis=1, keepdims=True) / float(d))
        row_ref[r, :] = rn
        acc[...] += sq
        wacc[...] += g2 * (1.0 / rn)
        return carry

    lax.fori_loop(0, rows // 8, stat_step, 0)
    pa = jnp.sum(acc[...], axis=0, keepdims=True)
    pw = jnp.sum(wacc[...], axis=0, keepdims=True)
    q = d // 4
    for j in range(4):
        statz[z, j : j + 1, :] = pa[:, j * q : (j + 1) * q]
        statz[z, 4 + j : 5 + j, :] = pw[:, j * q : (j + 1) * q]
    wsend[...] = jnp.zeros_like(wsend)
    for k in range(NC):
        for m in range(4):
            wfull[k, m * kp + 2 * rp : (m + 1) * kp, :] = jnp.zeros((kp - 2 * rp, cw), wfull.dtype)

    stz = [
        copy(statz.at[z], statz.at[z], s_statz.at[k], r_statz.at[k], dev(z_=zz))
        for k, zz in enumerate(zpeers)
    ]
    for s in stz:
        s.start()
    for h in hz[1:]:
        h.start()
    for s in stz:
        s.wait()
    total = ((statz[0] + statz[1]) + statz[2]) + statz[3]
    for k, to in enumerate((dev(mp_=flip(1, 0)), dev(x_=1 - x), dev(mp_=flip(0, 1)))):
        statp[k, 0] = total
        s = copy(statp.at[k, 0], statp.at[k, 1], s_statp.at[k], r_statp.at[k], to)
        s.start()
        s.wait()
        total = total + statp[k, 1]
    for j in range(4):
        cols = slice(j * q, (j + 1) * q)
        col_ref[:, cols] = KEEP * cf_ref[:, cols] + (1.0 - KEEP) * total[j : j + 1, :] / float(ffw)
        acc[0:1, cols] = total[4 + j : 5 + j, :]
    square_total = jnp.sum(acc[0:1, :] / col_ref[...], axis=1, keepdims=True)
    root_mean = jnp.sqrt(square_total / float(ffw * d))
    mult[...] = 1.0 / jnp.maximum(1.0, root_mean)

    def rows_of(m):
        return pl.ds(pl.multiple_of(m * kp + x * rp, 16), rp)

    def w_copy(k, n):
        if n < 3:
            j = flip(*turns[n])
            src, dst, to = wsend.at[k, j], wfull.at[k, rows_of(mp), :], dev(mp_=j)
        elif n == 3:
            src, dst, to = wsend.at[k, mp], wfull.at[k, rows_of(mp), :], dev(x_=1 - x)
        else:
            part = wfull.at[k, rows_of(flip(*turns[n - 4])), :]
            src, dst, to = part, part, dev(x_=1 - x)
        return copy(src, dst, s_w.at[k, n], r_w.at[k, n], to)

    def weights(k):
        def block(j, carry):
            cols = pl.ds(pl.multiple_of(j * nb + k * cw, 128), cw)
            scaled = grad_ref[:, cols] * lax.rsqrt(row_ref[...] * col_ref[:, cols])
            u = scaled * mult[...]
            upd_ref[:, cols] = u
            wsend[k, j, 0:rows, :] = (master_ref[:, cols] - RATE * u).astype(jnp.bfloat16)
            return carry

        lax.fori_loop(0, 4, block, 0)
        for n in range(4):
            w_copy(k, n).start()
        wfull[k, rows_of(mp), :] = wsend[k, mp]

    def forward(k):
        for n in range(3):
            w_copy(k, n).wait_recv()
            w_copy(k, 4 + n).start()

    weights(0)
    relay(1)
    weights(1)
    forward(0)
    relay(2)
    weights(2)
    forward(1)
    relay(3)
    weights(3)
    forward(2)
    other_lane = pl.ds(pl.multiple_of(flip(1, 0) * kp, 128), kp)
    for k, t in enumerate(order):
        hy[k].wait_recv()
        part = hfull.at[t, :, other_lane]
        hc.append(copy(part, part, s_hc.at[1, k], r_hc.at[1, k], dev(mp_=flip(0, 1))))
        hc[-1].start()
    for h in hc:
        h.wait_recv()

    def product(k, t):
        return jnp.dot(hfull[t], wfull[k], preferred_element_type=jnp.float32)

    def p_copy(k, way, dist):
        step = 1 if way == 0 else -1
        slot = way * 3 + (dist - 1)
        land = slot
        return copy(
            psend.at[k, slot], precv.at[k, land], s_p.at[k, slot], r_p.at[k, land],
            dev(z_=jnp.clip(z + step, 0, NZ - 1)),
        )

    def p_wait(k, way, dist):
        slot = way * 3 + dist - 1
        copy(psend.at[k, slot], precv.at[k, slot], s_p.at[k, slot], r_p.at[k, slot], dev(z_=(z + 1) % NZ)).wait_recv()

    def inside(way, dist):
        return z + dist <= NZ - 1 if way == 0 else z - dist >= 0

    def has_before(way):
        return z > 0 if way == 0 else z < NZ - 1

    def send_step(k, carry):
        for n in range(3, 7):
            w_copy(k, n).wait_recv()
        for dist in range(NZ - 1, 0, -1):
            for way in range(2):
                @pl.when(inside(way, dist))
                def _():
                    t = z + dist if way == 0 else z - dist
                    part = product(k, t)
                    slot = way * 3 + dist - 1
                    if dist < NZ - 1:
                        @pl.when(has_before(way))
                        def _():
                            p_wait(k, way, dist + 1)
                            psend[k, slot] = (part + precv[k, slot + 1].astype(jnp.float32)).astype(jnp.bfloat16)

                        @pl.when(jnp.logical_not(has_before(way)))
                        def _():
                            psend[k, slot] = part.astype(jnp.bfloat16)
                    else:
                        psend[k, slot] = part.astype(jnp.bfloat16)
                    p_copy(k, way, dist).start()

        @pl.when(k == 0)
        def _():
            forward(NC - 1)

        return carry

    lax.fori_loop(0, NC, send_step, 0)

    for k in range(NC):
        cols = slice(k * cw, (k + 1) * cw)
        acc2 = product(k, z)
        for way in range(2):
            @pl.when(has_before(way))
            def _():
                p_wait(k, way, 1)

            acc2 = acc2 + jnp.where(has_before(way), precv[k, way * 3].astype(jnp.float32), 0.0)
        out_ref[:, cols] = acc2.astype(out_ref.dtype)

    def drain(k, carry):
        for n in range(7):
            w_copy(k, n).wait_send()
        for dist in range(NZ - 1, 0, -1):
            for way in range(2):
                @pl.when(inside(way, dist))
                def _():
                    p_copy(k, way, dist).wait_send()
        return carry

    lax.fori_loop(0, NC, drain, 0)
    for h in hz + hy + hc:
        h.wait_send()


def fast_body(hidden, master, grad, row_factor, col_factor):
    tok, kin = hidden.shape
    rows, d = grad.shape
    rp = up(rows, 16)
    kp = up(NX * rp, 128)
    nb = d // 4
    cw = nb // NC
    h = hidden.reshape(tok, NZ, NX, rows)
    h = jnp.pad(h, ((0, 0), (0, 0), (0, 0), (0, rp - rows))).reshape(tok, NZ, NX * rp)
    h = jnp.pad(h, ((0, 0), (0, 0), (0, kp - NX * rp))).transpose(1, 0, 2)
    dma = pltpu.SemaphoreType.DMA
    bf, f32 = jnp.bfloat16, jnp.float32
    vmem = pl.BlockSpec(memory_space=pltpu.VMEM)
    out, upd, row, col = pl.pallas_call(
        kernel,
        out_shape=(
            jax.ShapeDtypeStruct((tok, nb), bf),
            jax.ShapeDtypeStruct((rows, d), f32),
            jax.ShapeDtypeStruct((rows, 1), f32),
            jax.ShapeDtypeStruct((1, d), f32),
        ),
        in_specs=[vmem] * 5,
        out_specs=(vmem,) * 4,
        scratch_shapes=[
            pltpu.VMEM((NZ, tok, 4 * kp), bf),
            pltpu.VMEM((NC, 4, rp, cw), bf),
            pltpu.VMEM((NC, 4 * kp, cw), bf),
            pltpu.VMEM((8, d), f32),
            pltpu.VMEM((8, d), f32),
            pltpu.VMEM((NZ, 8, d // 4), f32),
            pltpu.VMEM((3, 2, 8, d // 4), f32),
            pltpu.VMEM((1, 1), f32),
            pltpu.VMEM((NC, 6, tok, cw), bf),
            pltpu.VMEM((NC, 6, tok, cw), bf),
            dma((3,)), dma((3,)), dma((3,)), dma((3,)),
            dma((3,)), dma((3,)), dma((4,)), dma((4,)), dma((2, 4)), dma((2, 4)),
            dma((NC, 7)), dma((NC, 7)), dma((NC, 6)), dma((NC, 6)),
        ],
        compiler_params=pltpu.CompilerParams(
            collective_id=0, has_side_effects=True, vmem_limit_bytes=60 * 1024 * 1024
        ),
    )(h, master, grad, row_factor[:, None], col_factor[None, :])
    return out, upd, row[:, 0], col[0]


def plain_body(hidden, master, grad, row_factor, col_factor):
    squared = grad * grad + 1e-30
    row_new = KEEP * row_factor + (1.0 - KEEP) * jnp.mean(squared, axis=1)
    column_part = jnp.sum(squared, axis=0)
    weighted_part = jnp.sum(grad * grad / row_new[:, None], axis=0)
    column_total, weighted_total = lax.psum((column_part, weighted_part), ("dp", "mp"))
    col_new = KEEP * col_factor + (1.0 - KEEP) * column_total / float(FFW)
    scaled = grad * lax.rsqrt(row_new[:, None] * col_new[None, :])
    root_mean = jnp.sqrt(jnp.sum(weighted_total / col_new) / float(FFW * D))
    update = scaled / jnp.maximum(1.0, root_mean)
    weight = (master - RATE * update).astype(jnp.bfloat16)
    partial_out = jnp.dot(
        hidden, lax.all_gather(weight, "dp", axis=0, tiled=True), preferred_element_type=jnp.float32
    )
    ffn_out = lax.psum_scatter(partial_out, "mp", scatter_dimension=1, tiled=True)
    return ffn_out.astype(jnp.bfloat16), update, row_new, col_new


def solution(mesh):
    fits = mesh.shape["dp"] == NX * NZ and mesh.shape["mp"] == 4
    return jax.shard_map(
        fast_body if fits else plain_body,
        mesh=mesh,
        in_specs=(
            P("dp", "mp"),
            P(("mp", "dp"), None),
            P(("mp", "dp"), None),
            P(("mp", "dp")),
            P(),
        ),
        out_specs=(P("dp", "mp"), P(("mp", "dp"), None), P(("mp", "dp")), P()),
        check_vma=False,
    )
```

```python
import functools

import jax
import jax.numpy as jnp
from jax import lax
from jax.experimental import pallas as pl
from jax.experimental.pallas import tpu as pltpu
from jax.sharding import PartitionSpec as P

D = 4096
FFW = 5376
STEP = 10
KEEP = 1.0 - STEP ** (-0.8)
RATE = min(0.01, STEP ** (-0.5))
MESH = pl.DeviceIdType.MESH
NX = 2
NZ = 4
NC = 4


def up(n, m):
    return (n + m - 1) // m * m


def kernel(
    hid_ref, master_ref, grad_ref, rf_ref, cf_ref,
    out_ref, upd_ref, row_ref, col_ref,
    hfull, wsend, wfull, acc, wacc, statz, statp, mult, psend, precv, own,
    s_statz, r_statz, s_statp, r_statp, s_hz, r_hz, s_hy, r_hy, s_hc, r_hc, s_w, r_w, s_p, r_p,
):
    rows, d = grad_ref.shape
    tok = hid_ref.shape[1]
    kp = hid_ref.shape[2]
    rp = wsend.shape[2]
    cw = wsend.shape[3]
    nb = NC * cw
    ffw = rows * NX * NZ * 4
    dp = lax.axis_index("dp")
    mp = lax.axis_index("mp")
    z, x = dp // NX, dp % NX
    y, c = mp // 2, mp % 2

    def dev(z_=None, x_=None, mp_=None):
        z_ = z if z_ is None else z_
        x_ = x if x_ is None else x_
        mp_ = mp if mp_ is None else mp_
        return {"dp": z_ * NX + x_, "mp": mp_}

    def flip(dy, dc):
        return (y + dy) % 2 * 2 + (c + dc) % 2

    def copy(src, dst, ssem, rsem, to):
        return pltpu.make_async_remote_copy(
            src_ref=src, dst_ref=dst, send_sem=ssem, recv_sem=rsem, device_id=to, device_id_type=MESH
        )

    zpeers = [(z + k) % NZ for k in range(1, NZ)]
    turns = [(0, 1), (1, 0), (1, 1)]
    barrier = pltpu.get_barrier_semaphore()
    for zz in zpeers:
        pl.semaphore_signal(barrier, inc=1, device_id=dev(z_=zz), device_id_type=MESH)
    for turn in turns:
        pl.semaphore_signal(barrier, inc=1, device_id=dev(mp_=flip(*turn)), device_id_type=MESH)
    pl.semaphore_signal(barrier, inc=1, device_id=dev(x_=1 - x), device_id_type=MESH)

    my_lane = pl.ds(pl.multiple_of(mp * kp, 128), kp)
    hfull[z, :, my_lane] = hid_ref[z]
    order = [z] + [(z - k) % NZ for k in range(1, NZ)]
    hz = [
        copy(hid_ref.at[zz], hfull.at[z, :, my_lane], s_hz.at[k], r_hz.at[k], dev(z_=zz))
        for k, zz in enumerate(zpeers)
    ]
    hy, hc = [], []

    def relay(k):
        if k:
            hz[k - 1].wait_recv()
        part = hfull.at[order[k], :, my_lane]
        hy.append(copy(part, part, s_hy.at[k], r_hy.at[k], dev(mp_=flip(1, 0))))
        hc.append(copy(part, part, s_hc.at[0, k], r_hc.at[0, k], dev(mp_=flip(0, 1))))
        hy[-1].start()
        hc[-1].start()

    pl.semaphore_wait(barrier, NZ - 1 + 4)
    hz[0].start()
    relay(0)

    acc[...] = jnp.zeros_like(acc)
    wacc[...] = jnp.zeros_like(wacc)

    def stat_step(i, carry):
        r = pl.ds(pl.multiple_of(i * 8, 8), 8)
        g = grad_ref[r, :]
        g2 = g * g
        sq = g2 + 1e-30
        rn = KEEP * rf_ref[r, :] + (1.0 - KEEP) * (jnp.sum(sq, axis=1, keepdims=True) / float(d))
        row_ref[r, :] = rn
        acc[...] += sq
        wacc[...] += g2 * (1.0 / rn)
        return carry

    lax.fori_loop(0, rows // 8, stat_step, 0)
    pa = jnp.sum(acc[...], axis=0, keepdims=True)
    pw = jnp.sum(wacc[...], axis=0, keepdims=True)
    q = d // 4
    for j in range(4):
        statz[z, j : j + 1, :] = pa[:, j * q : (j + 1) * q]
        statz[z, 4 + j : 5 + j, :] = pw[:, j * q : (j + 1) * q]
    wsend[...] = jnp.zeros_like(wsend)
    for k in range(NC):
        for m in range(4):
            wfull[k, m * kp + 2 * rp : (m + 1) * kp, :] = jnp.zeros((kp - 2 * rp, cw), wfull.dtype)

    stz = [
        copy(statz.at[z], statz.at[z], s_statz.at[k], r_statz.at[k], dev(z_=zz))
        for k, zz in enumerate(zpeers)
    ]
    for s in stz:
        s.start()
    for h in hz[1:]:
        h.start()
    for s in stz:
        s.wait()
    total = ((statz[0] + statz[1]) + statz[2]) + statz[3]
    for k, to in enumerate((dev(mp_=flip(1, 0)), dev(x_=1 - x), dev(mp_=flip(0, 1)))):
        statp[k, 0] = total
        s = copy(statp.at[k, 0], statp.at[k, 1], s_statp.at[k], r_statp.at[k], to)
        s.start()
        s.wait()
        total = total + statp[k, 1]
    for j in range(4):
        cols = slice(j * q, (j + 1) * q)
        col_ref[:, cols] = KEEP * cf_ref[:, cols] + (1.0 - KEEP) * total[j : j + 1, :] / float(ffw)
        acc[0:1, cols] = total[4 + j : 5 + j, :]
    square_total = jnp.sum(acc[0:1, :] / col_ref[...], axis=1, keepdims=True)
    root_mean = jnp.sqrt(square_total / float(ffw * d))
    mult[...] = 1.0 / jnp.maximum(1.0, root_mean)

    def rows_of(m):
        return pl.ds(pl.multiple_of(m * kp + x * rp, 16), rp)

    def w_copy(k, n):
        if n < 3:
            j = flip(*turns[n])
            src, dst, to = wsend.at[k, j], wfull.at[k, rows_of(mp), :], dev(mp_=j)
        elif n == 3:
            src, dst, to = wsend.at[k, mp], wfull.at[k, rows_of(mp), :], dev(x_=1 - x)
        else:
            part = wfull.at[k, rows_of(flip(*turns[n - 4])), :]
            src, dst, to = part, part, dev(x_=1 - x)
        return copy(src, dst, s_w.at[k, n], r_w.at[k, n], to)

    def weights(k):
        def block(j, carry):
            cols = pl.ds(pl.multiple_of(j * nb + k * cw, 128), cw)
            scaled = grad_ref[:, cols] * lax.rsqrt(row_ref[...] * col_ref[:, cols])
            u = scaled * mult[...]
            upd_ref[:, cols] = u
            wsend[k, j, 0:rows, :] = (master_ref[:, cols] - RATE * u).astype(jnp.bfloat16)
            return carry

        lax.fori_loop(0, 4, block, 0)
        for n in range(4):
            w_copy(k, n).start()
        wfull[k, rows_of(mp), :] = wsend[k, mp]

    def forward(k):
        for n in range(3):
            w_copy(k, n).wait_recv()
            w_copy(k, 4 + n).start()

    weights(0)
    relay(1)
    weights(1)
    forward(0)
    relay(2)
    weights(2)
    forward(1)
    relay(3)
    weights(3)
    forward(2)
    other_lane = pl.ds(pl.multiple_of(flip(1, 0) * kp, 128), kp)
    for k, t in enumerate(order):
        hy[k].wait_recv()
        part = hfull.at[t, :, other_lane]
        hc.append(copy(part, part, s_hc.at[1, k], r_hc.at[1, k], dev(mp_=flip(0, 1))))
        hc[-1].start()
    for h in hc:
        h.wait_recv()

    def product(k, t):
        return jnp.dot(hfull[t], wfull[k], preferred_element_type=jnp.float32)

    def p_copy(k, way, dist):
        step = 1 if way == 0 else -1
        slot = way * 3 + (dist - 1)
        land = slot
        return copy(
            psend.at[k, slot], precv.at[k, land], s_p.at[k, slot], r_p.at[k, land],
            dev(z_=jnp.clip(z + step, 0, NZ - 1)),
        )

    def p_wait(k, way, dist):
        slot = way * 3 + dist - 1
        copy(psend.at[k, slot], precv.at[k, slot], s_p.at[k, slot], r_p.at[k, slot], dev(z_=(z + 1) % NZ)).wait_recv()

    def inside(way, dist):
        return z + dist <= NZ - 1 if way == 0 else z - dist >= 0

    def has_before(way):
        return z > 0 if way == 0 else z < NZ - 1

    def send_step(k, carry):
        for n in range(3, 7):
            w_copy(k, n).wait_recv()
        for dist in range(NZ - 1, 0, -1):
            for way in range(2):
                @pl.when(inside(way, dist))
                def _():
                    t = z + dist if way == 0 else z - dist
                    part = product(k, t)
                    slot = way * 3 + dist - 1
                    if dist < NZ - 1:
                        @pl.when(has_before(way))
                        def _():
                            p_wait(k, way, dist + 1)
                            psend[k, slot] = (part + precv[k, slot + 1].astype(jnp.float32)).astype(jnp.bfloat16)

                        @pl.when(jnp.logical_not(has_before(way)))
                        def _():
                            psend[k, slot] = part.astype(jnp.bfloat16)
                    else:
                        psend[k, slot] = part.astype(jnp.bfloat16)
                    p_copy(k, way, dist).start()

        @pl.when(k == 0)
        def _():
            forward(NC - 1)

        own[k] = product(k, z)
        return carry

    lax.fori_loop(0, NC, send_step, 0)

    for k in range(NC):
        cols = slice(k * cw, (k + 1) * cw)
        acc2 = own[k]
        for way in range(2):
            @pl.when(has_before(way))
            def _():
                p_wait(k, way, 1)

            acc2 = acc2 + jnp.where(has_before(way), precv[k, way * 3].astype(jnp.float32), 0.0)
        out_ref[:, cols] = acc2.astype(out_ref.dtype)

    def drain(k, carry):
        for n in range(7):
            w_copy(k, n).wait_send()
        for dist in range(NZ - 1, 0, -1):
            for way in range(2):
                @pl.when(inside(way, dist))
                def _():
                    p_copy(k, way, dist).wait_send()
        return carry

    lax.fori_loop(0, NC, drain, 0)
    for h in hz + hy + hc:
        h.wait_send()


def fast_body(hidden, master, grad, row_factor, col_factor):
    tok, kin = hidden.shape
    rows, d = grad.shape
    rp = up(rows, 16)
    kp = up(NX * rp, 128)
    nb = d // 4
    cw = nb // NC
    h = hidden.reshape(tok, NZ, NX, rows)
    h = jnp.pad(h, ((0, 0), (0, 0), (0, 0), (0, rp - rows))).reshape(tok, NZ, NX * rp)
    h = jnp.pad(h, ((0, 0), (0, 0), (0, kp - NX * rp))).transpose(1, 0, 2)
    dma = pltpu.SemaphoreType.DMA
    bf, f32 = jnp.bfloat16, jnp.float32
    vmem = pl.BlockSpec(memory_space=pltpu.VMEM)
    out, upd, row, col = pl.pallas_call(
        kernel,
        out_shape=(
            jax.ShapeDtypeStruct((tok, nb), bf),
            jax.ShapeDtypeStruct((rows, d), f32),
            jax.ShapeDtypeStruct((rows, 1), f32),
            jax.ShapeDtypeStruct((1, d), f32),
        ),
        in_specs=[vmem] * 5,
        out_specs=(vmem,) * 4,
        scratch_shapes=[
            pltpu.VMEM((NZ, tok, 4 * kp), bf),
            pltpu.VMEM((NC, 4, rp, cw), bf),
            pltpu.VMEM((NC, 4 * kp, cw), bf),
            pltpu.VMEM((8, d), f32),
            pltpu.VMEM((8, d), f32),
            pltpu.VMEM((NZ, 8, d // 4), f32),
            pltpu.VMEM((3, 2, 8, d // 4), f32),
            pltpu.VMEM((1, 1), f32),
            pltpu.VMEM((NC, 6, tok, cw), bf),
            pltpu.VMEM((NC, 6, tok, cw), bf),
            pltpu.VMEM((NC, tok, cw), f32),
            dma((3,)), dma((3,)), dma((3,)), dma((3,)),
            dma((3,)), dma((3,)), dma((4,)), dma((4,)), dma((2, 4)), dma((2, 4)),
            dma((NC, 7)), dma((NC, 7)), dma((NC, 6)), dma((NC, 6)),
        ],
        compiler_params=pltpu.CompilerParams(
            collective_id=0, has_side_effects=True, vmem_limit_bytes=60 * 1024 * 1024
        ),
    )(h, master, grad, row_factor[:, None], col_factor[None, :])
    return out, upd, row[:, 0], col[0]


def plain_body(hidden, master, grad, row_factor, col_factor):
    squared = grad * grad + 1e-30
    row_new = KEEP * row_factor + (1.0 - KEEP) * jnp.mean(squared, axis=1)
    column_part = jnp.sum(squared, axis=0)
    weighted_part = jnp.sum(grad * grad / row_new[:, None], axis=0)
    column_total, weighted_total = lax.psum((column_part, weighted_part), ("dp", "mp"))
    col_new = KEEP * col_factor + (1.0 - KEEP) * column_total / float(FFW)
    scaled = grad * lax.rsqrt(row_new[:, None] * col_new[None, :])
    root_mean = jnp.sqrt(jnp.sum(weighted_total / col_new) / float(FFW * D))
    update = scaled / jnp.maximum(1.0, root_mean)
    weight = (master - RATE * update).astype(jnp.bfloat16)
    partial_out = jnp.dot(
        hidden, lax.all_gather(weight, "dp", axis=0, tiled=True), preferred_element_type=jnp.float32
    )
    ffn_out = lax.psum_scatter(partial_out, "mp", scatter_dimension=1, tiled=True)
    return ffn_out.astype(jnp.bfloat16), update, row_new, col_new


def solution(mesh):
    fits = mesh.shape["dp"] == NX * NZ and mesh.shape["mp"] == 4
    return jax.shard_map(
        fast_body if fits else plain_body,
        mesh=mesh,
        in_specs=(
            P("dp", "mp"),
            P(("mp", "dp"), None),
            P(("mp", "dp"), None),
            P(("mp", "dp")),
            P(),
        ),
        out_specs=(P("dp", "mp"), P(("mp", "dp"), None), P(("mp", "dp")), P()),
        check_vma=False,
    )
```
